16 devices in a mesh: rep: 1, dp: 16 (over x, y, z, core).
Axes of the slice: x: 2, y: 2, z: 2, core: 2. Of those that a mesh axis runs over, the one named last changes fastest.
Arguments:
- x: bfloat16 [16, 2048, 1280], P(('rep', 'dp'))
- dy: bfloat16 [16, 2048, 1280], P(('rep', 'dp'))
- w_gate: bfloat16 [2, 1280, 5120], P(None, 'dp')
- w_up: bfloat16 [2, 1280, 5120], P(None, 'dp')
- w_down: bfloat16 [2, 5120, 1280], P(None, 'dp')
- m_w_gate: float32 [2, 1280, 5120], P(None, 'dp')
- m_w_up: float32 [2, 1280, 5120], P(None, 'dp')
- m_w_down: float32 [2, 5120, 1280], P(None, 'dp')
- v_w_gate: float32 [2, 1280, 5120], P(None, 'dp')
- v_w_up: float32 [2, 1280, 5120], P(None, 'dp')
- v_w_down: float32 [2, 5120, 1280], P(None, 'dp')
Outputs:
- output 1: bfloat16 [2, 1280, 5120], P('rep', 'dp')
- output 2: bfloat16 [2, 1280, 5120], P('rep', 'dp')
- output 3: bfloat16 [2, 5120, 1280], P('rep', 'dp')
- output 4: float32 [2, 1280, 5120], P('rep', 'dp')
- output 5: float32 [2, 1280, 5120], P('rep', 'dp')
- output 6: float32 [2, 5120, 1280], P('rep', 'dp')
- output 7: float32 [2, 1280, 5120], P('rep', 'dp')
- output 8: float32 [2, 1280, 5120], P('rep', 'dp')
- output 9: float32 [2, 5120, 1280], P('rep', 'dp')
All inputs are finite; a program needn't handle non-finite values.
Results may differ from the reference program's by a relative error of at most 0.0224.
Values are sent between devices in bfloat16 or wider.
A program may use at most 2 GiB of HBM per device.

```python
import jax
import jax.numpy as jnp
from jax import lax

SEQUENCES = 16
TOKENS = 2048
D = 1280
FF = 5120
LAYERS = 2
NAMES = ("w_gate", "w_up", "w_down")
SHAPES = {"w_gate": (LAYERS, D, FF), "w_up": (LAYERS, D, FF), "w_down": (LAYERS, FF, D)}


def bump(key, n, height):
    away = (jnp.arange(n, dtype=jnp.int32) - jax.random.randint(key, (), 0, n, jnp.int32)) % n
    return jnp.where(away < n // 8, height, 1.0)


def together(key, own, strength):
    shared = jax.random.normal(key, own.shape[1:], jnp.float32)
    return (own + strength * shared) * lax.rsqrt(1 + strength * strength)


def setup_inputs(seed: int = 0, part: int = 0) -> dict:
    kx, kdy, ka, kb, kz, kf, kh, kl, *keys = jax.random.split(jax.random.key(seed), 8 + 3 * len(NAMES))
    kx, kdy, ka, kb = (jax.random.fold_in(k, part) for k in (kx, kdy, ka, kb))
    kw, km, kv = (keys[i::3] for i in range(3))
    shape = (SEQUENCES, TOKENS, D)
    much_x, much_dy = jax.random.uniform(kz, (2,), jnp.float32, 0.0, 1.0)
    loud = 2.0 ** jax.random.uniform(jax.random.fold_in(kz, 1), (), jnp.float32, -1.0, 2.0)
    layers = 2.0 ** jax.random.uniform(kl, (LAYERS, 1, 1), jnp.float32, -1.0, 1.0)
    x = together(ka, jax.random.normal(kx, shape, jnp.float32), much_x) * bump(kf, D, 4.0)
    dy = together(kb, jax.random.normal(kdy, shape, jnp.float32), much_dy)
    drawn = {"x": x.astype(jnp.bfloat16), "dy": (loud * dy * (SEQUENCES * TOKENS) ** -0.5).astype(jnp.bfloat16)}
    for key, name in zip(kw, NAMES, strict=True):
        w = jax.random.normal(key, SHAPES[name], jnp.float32) * SHAPES[name][1] ** -0.5
        drawn[name] = (w * {"w_gate": 1.0, "w_up": bump(kh, FF, 4.0), "w_down": layers}[name]).astype(jnp.bfloat16)
    for key, name in zip(km, NAMES, strict=True):
        drawn[f"m_{name}"] = 0.1 * jax.random.normal(key, SHAPES[name], jnp.float32)
    for key, name in zip(kv, NAMES, strict=True):
        drawn[f"v_{name}"] = jax.random.uniform(key, SHAPES[name], jnp.float32, 0.005, 0.015)
    return drawn


def matmul(a, w):
    return jnp.dot(a, w, preferred_element_type=jnp.float32).astype(jnp.bfloat16)


def normed(h):
    wide = h.astype(jnp.float32)
    scale = lax.rsqrt(jnp.mean(wide**2, -1, keepdims=True) + 1e-6)
    return (wide * scale).astype(jnp.bfloat16)


def layer(h, w):
    a = normed(h)
    gate = jnp.dot(a, w["w_gate"], preferred_element_type=jnp.float32)
    up = jnp.dot(a, w["w_up"], preferred_element_type=jnp.float32)
    return h + matmul((jax.nn.silu(gate) * up).astype(jnp.bfloat16), w["w_down"])


def adamw(w, m, v, g):
    m = 0.9 * m + 0.1 * g
    v = 0.95 * v + 0.05 * g * g
    step = m * lax.rsqrt(v + 1e-8) + 0.1 * w
    return (w - 0.02 * step).astype(jnp.bfloat16), m, v


def clipped(gradients, sum_of_squares, count):
    factor = jnp.minimum(1.0, 0.5 * lax.rsqrt(sum_of_squares / count + 1e-30))
    return [g * factor for g in gradients]


def stack(weights, h):
    return lax.scan(lambda h, w: (layer(h, w), None), h, weights)[0]


def reference(x, dy, w_gate, w_up, w_down, m_w_gate, m_w_up, m_w_down, v_w_gate, v_w_up, v_w_down):
    weights = dict(zip(NAMES, (w_gate, w_up, w_down), strict=True))

    def take(so_far, sequence):
        h, by_y = sequence
        _, back = jax.vjp(lambda w: stack(w, h), weights)
        return jax.tree.map(lambda total, term: total + term.astype(jnp.float32), so_far, back(by_y)[0]), None

    none_yet = {name: jnp.zeros(w.shape, jnp.float32) for name, w in weights.items()}
    by_weights, _ = lax.scan(take, none_yet, (x, dy))
    gradients = [by_weights[name].astype(jnp.bfloat16).astype(jnp.float32) for name in NAMES]
    gradients = clipped(gradients, sum(jnp.sum(g * g) for g in gradients), sum(g.size for g in gradients))
    new = [
        adamw(w.astype(jnp.float32), m, v, g)
        for w, m, v, g in zip((w_gate, w_up, w_down), (m_w_gate, m_w_up, m_w_down), (v_w_gate, v_w_up, v_w_down), gradients, strict=True)
    ]
    return tuple(one[which] for which in range(3) for one in new)
```

```python
import jax
import jax.numpy as jnp
from jax import lax
from jax.experimental import pallas as pl
from jax.experimental.pallas import tpu as pltpu
from jax.sharding import PartitionSpec as P

F32, BF16 = jnp.float32, jnp.bfloat16


def normed(h):
    wide = h.astype(F32)
    scale = lax.rsqrt(jnp.mean(wide**2, -1, keepdims=True) + 1e-6)
    return (wide * scale).astype(BF16)


def adamw(w, m, v, g):
    m = 0.9 * m + 0.1 * g
    v = 0.95 * v + 0.05 * g * g
    step = m * lax.rsqrt(v + 1e-8) + 0.1 * w
    return (w - 0.02 * step).astype(BF16), m, v


def dot(a, b, contract):
    return lax.dot_general(a, b, ((contract[:1], contract[1:]), ((), ())), preferred_element_type=F32)


def everywhere(n, part):
    def kernel(part_ref, out_ref, slots, send_sem, recv_sem):
        me = lax.axis_index("dp")
        barrier = pltpu.get_barrier_semaphore()
        for k in range(1, n):
            pl.semaphore_signal(barrier, inc=1, device_id={"dp": lax.rem(me + k, n)}, device_id_type=pl.DeviceIdType.MESH)
        pl.semaphore_wait(barrier, n - 1)
        copies = []
        for k in range(1, n):
            copy = pltpu.make_async_remote_copy(
                src_ref=part_ref,
                dst_ref=slots.at[k],
                send_sem=send_sem.at[k],
                recv_sem=recv_sem.at[k],
                device_id={"dp": lax.rem(me + k, n)},
                device_id_type=pl.DeviceIdType.MESH,
            )
            copy.start()
            copies.append(copy)
        total = part_ref[...]
        for k, copy in enumerate(copies, 1):
            copy.wait()
            total = total + slots[k]
        out_ref[...] = total

    return pl.pallas_call(
        kernel,
        out_shape=jax.ShapeDtypeStruct((8, 128), F32),
        in_specs=[pl.BlockSpec(memory_space=pltpu.VMEM)],
        out_specs=pl.BlockSpec(memory_space=pltpu.VMEM),
        scratch_shapes=[pltpu.VMEM((n, 8, 128), F32), pltpu.SemaphoreType.DMA((n,)), pltpu.SemaphoreType.DMA((n,))],
        compiler_params=pltpu.CompilerParams(collective_id=0, has_side_effects=True),
    )(part)


class Gather:
    SENDS = [(0, 8), (0, 4), (0, 2), (8, 4), (4, 2), (2, 8), (12, 2), (6, 8), (10, 4)]
    HANDED = [0, 8, 4, 2, 12, 6, 10, 14]
    COPIES = 17

    def __init__(self, shard, full, send_sem, recv_sem, local_sem):
        me = lax.axis_index("dp")
        rows, cols = shard.shape
        unit = cols // 128
        first, later = unit - unit // 3 * 2, unit // 3
        thirds = [(0, first * 128), (first * 128, later * 128), ((first + later) * 128, later * 128)]

        def flip(bits):
            for bit in (8, 4, 2, 1):
                if bits & bit:
                    yield bit

        def at(bits):
            owner = me
            for bit in flip(bits):
                owner = owner + bit - 2 * bit * (owner // bit % 2)
            return owner

        def block(bits, third=None):
            start = pl.multiple_of(at(bits) * rows, 16)
            if third is None:
                return full.at[pl.ds(start, rows), :]
            return full.at[pl.ds(start, rows), pl.ds(thirds[third][0], thirds[third][1])]

        def copy(k, bits, to, third=None):
            return pltpu.make_async_remote_copy(
                src_ref=shard if bits == 0 else block(bits, third),
                dst_ref=block(bits, third),
                send_sem=send_sem.at[k],
                recv_sem=recv_sem.at[k],
                device_id={"dp": at(to)},
                device_id_type=pl.DeviceIdType.MESH,
            )

        self.far = [copy(k, bits, to, k - 6 if k >= 6 else None) for k, (bits, to) in enumerate(self.SENDS)]
        self.near = [copy(9 + k, bits, 1) for k, bits in enumerate(self.HANDED)]
        self.local = pltpu.make_async_copy(shard, block(0), local_sem)

    def phase(self, number):
        if number == 0:
            for copy in self.far[:3] + self.near[:1] + [self.local]:
                copy.start()
        elif number < 3:
            for k in range(3 * number - 3, 3 * number):
                self.far[k].wait_recv()
                self.far[k + 3].start()
                self.near[k + 1].start()
        elif number == 3:
            for k in range(6, 9):
                self.far[k].wait_recv()
            self.near[7].start()
        else:
            for copy in self.near:
                copy.wait_recv()
            for copy in self.far + self.near:
                copy.wait_send()
            self.local.wait()


def meet():
    me = lax.axis_index("dp")
    barrier = pltpu.get_barrier_semaphore()
    for bit in (8, 4, 2, 1):
        other = me + bit - 2 * bit * (me // bit % 2)
        pl.semaphore_signal(barrier, inc=1, device_id={"dp": other}, device_id_type=pl.DeviceIdType.MESH)
    pl.semaphore_wait(barrier, 4)


def hosting(body, steps, operands, in_specs, out_shape, out_specs, shards, when, identity, flops, moved):
    many, given, made = len(shards), len(operands), len(out_shape)

    def kernel(*refs):
        ins, rest = refs[:given], refs[given:]
        mine, rest = rest[:many], rest[many:]
        outs, rest = rest[:made], rest[made:]
        full, (send_sem, recv_sem, local_sem) = rest[:many], rest[many:]
        step = pl.program_id(0)
        gathers = [Gather(mine[i], full[i], send_sem.at[i], recv_sem.at[i], local_sem.at[i]) for i in range(many)]
        for now in range(steps):
            due = [(phase, i) for i in range(many) for phase in range(4) if when[i][phase] == now]
            if due:

                @pl.when(step == now)
                def _():
                    if now == 0:
                        meet()
                    for phase, i in sorted(due):
                        gathers[i].phase(phase)

        if body is not None:
            body(*ins, *outs)

        @pl.when(step == steps - 1)
        def _():
            for gather in gathers:
                gather.phase(4)

    anywhere = [pl.BlockSpec(memory_space=pl.ANY)] * many
    whole = [jax.ShapeDtypeStruct((16 * one.shape[0], one.shape[1]), one.dtype) for one in shards]
    return pl.pallas_call(
        kernel,
        grid=(steps,),
        out_shape=list(out_shape) + whole,
        in_specs=list(in_specs) + anywhere,
        out_specs=list(out_specs) + anywhere,
        scratch_shapes=[
            pltpu.SemaphoreType.DMA((many, Gather.COPIES)),
            pltpu.SemaphoreType.DMA((many, Gather.COPIES)),
            pltpu.SemaphoreType.DMA((many,)),
        ],
        compiler_params=pltpu.CompilerParams(
            collective_id=identity, has_side_effects=True, dimension_semantics=("arbitrary",), vmem_limit_bytes=60 * 2**20
        ),
        cost_estimate=pl.CostEstimate(flops=flops, bytes_accessed=moved, transcendentals=0),
    )(*operands, *shards)


def gathered(shards, identity):
    when = [(0, 0, 0, 0)] * len(shards)
    return hosting(None, 1, [], [], [], [], shards, when, identity, 10**9, 10**8)


def hidden(a, w_gate, w_up, shards, when, identity):
    tokens, d = a.shape
    ff = w_gate.shape[1]
    wide = 256

    def body(a_ref, gate_w, up_w, gate_ref, up_ref, hid_ref):
        gate = jnp.dot(a_ref[...], gate_w[...], preferred_element_type=F32)
        up = jnp.dot(a_ref[...], up_w[...], preferred_element_type=F32)
        gate_ref[...] = gate
        up_ref[...] = up
        hid_ref[...] = (gate * jax.nn.sigmoid(gate) * up).astype(BF16)

    weight, out = pl.BlockSpec((d, wide), lambda j: (0, j)), pl.BlockSpec((tokens, wide), lambda j: (0, j))
    like = [jax.ShapeDtypeStruct((tokens, ff), t) for t in (F32, F32, BF16)]
    specs = [pl.BlockSpec((tokens, d), lambda j: (0, 0)), weight, weight]
    return hosting(body, ff // wide, [a, w_gate, w_up], specs, like, [out] * 3, shards, when, identity, 4 * tokens * d * ff, 150 * 2**20)


def lowered(hid, w_down, h, shards, when, identity):
    tokens, ff = hid.shape
    d = w_down.shape[1]
    tall = 256

    def body(hid_ref, w_ref, h_ref, out_ref):
        out_ref[...] = h_ref[...] + jnp.dot(hid_ref[...], w_ref[...], preferred_element_type=F32).astype(BF16)

    row = pl.BlockSpec((tall, d), lambda i: (i, 0))
    specs = [pl.BlockSpec((tall, ff), lambda i: (i, 0)), pl.BlockSpec((ff, d), lambda i: (0, 0)), row]
    like = [jax.ShapeDtypeStruct((tokens, d), BF16)]
    return hosting(body, tokens // tall, [hid, w_down, h], specs, like, [row], shards, when, identity, 2 * tokens * d * ff, 60 * 2**20)


def unhidden(by, w_down, gate, up):
    tokens, d = by.shape
    ff = w_down.shape[0]
    wide = 256

    def kernel(by_ref, w_ref, gate_ref, up_ref, by_gate, by_up):
        by_hid = lax.dot_general(by_ref[...], w_ref[...], (((1,), (1,)), ((), ())), preferred_element_type=F32).astype(BF16).astype(F32)
        gate = gate_ref[...]
        s = jax.nn.sigmoid(gate)
        by_up[...] = (by_hid * (gate * s)).astype(BF16)
        by_gate[...] = (by_hid * up_ref[...] * (s * (1 + gate * (1 - s)))).astype(BF16)

    block = pl.BlockSpec((tokens, wide), lambda j: (0, j))
    return pl.pallas_call(
        kernel,
        grid=(ff // wide,),
        out_shape=[jax.ShapeDtypeStruct((tokens, ff), BF16)] * 2,
        in_specs=[pl.BlockSpec((tokens, d), lambda j: (0, 0)), pl.BlockSpec((wide, d), lambda j: (j, 0)), block, block],
        out_specs=[block, block],
        compiler_params=pltpu.CompilerParams(dimension_semantics=("arbitrary",), vmem_limit_bytes=60 * 2**20),
        cost_estimate=pl.CostEstimate(flops=2 * tokens * d * ff, bytes_accessed=140 * 2**20, transcendentals=0),
    )(by, w_down, gate, up)


def solution(mesh):
    n = mesh.shape["dp"]
    names = {"x": 8, "y": 4, "z": 2, "core": 1}

    def swap(value, axis):
        return lax.ppermute(value, "dp", [(i, i ^ names[axis]) for i in range(n)])

    def pick(term, picks):
        array, had, (at, size) = term
        starts, sizes = [0, 0, 0, at, 0], list(array.shape[:3]) + [size, array.shape[4]]
        for d, bit in {**had, **picks}.items():
            if array.shape[d] > 1:
                starts[d], sizes[d] = bit, 1
        return lax.dynamic_slice(array, starts, sizes).astype(F32)

    def after(values, *earlier):
        return lax.optimization_barrier((values, earlier))[0]

    class Scattered:
        def __init__(self, a, b, cuts, core, bits):
            self.a, self.b, self.core, self.bits, self.cuts = a, b, core, bits, cuts
            self.half = b.shape[1] // 2

        def columns(self, core):
            return lax.dynamic_slice_in_dim(self.b, core * self.half, self.half, 1)

        def other(self, *earlier):
            self.a, self.b = after((self.a, self.b), *earlier)
            self.sent = dot(self.a, self.columns(1 - self.core), (0, 0)).astype(BF16)
            self.got = swap(self.sent, "core")
            return self.sent

        def own(self, *earlier):
            self.a, self.b = after((self.a, self.b), *earlier)
            own = dot(self.a, self.columns(self.core), (0, 0)) + self.got.astype(F32)
            rows = own.shape[0]
            own = own.reshape(2, 2, 2, rows // 8, self.half)
            at, self.parts = 0, []
            for size, order in self.cuts:
                self.parts.append(([(own, {}, (at, size))], order))
                at += size
            return own

        def halve(self, stage, *earlier):
            sends, parts = [], []
            for terms, order in self.parts:
                d = order[stage]
                held = [one[0] for one in terms]
                held = after(held, *earlier)
                terms = [(array, had, span) for array, (_, had, span) in zip(held, terms)]
                send = sum(pick(t, {d: 1 - self.bits[d]}) for t in terms).astype(BF16)
                got = swap(send, "xyz"[d])
                sends.append(send)
                terms = [(t, {**had, d: self.bits[d]}, span) for t, had, span in terms] + [(got, {}, (0, got.shape[3]))]
                parts.append((terms, order))
            self.parts = parts
            return sends

        def finish(self, *earlier):
            blocks = []
            for terms, _ in self.parts:
                held = after([one[0] for one in terms], *earlier)
                terms = [(array, had, span) for array, (_, had, span) in zip(held, terms)]
                blocks.append(sum(pick(t, {}) for t in terms)[0, 0, 0])
            block = jnp.concatenate(blocks).astype(BF16)
            self.squares = jnp.sum(block.astype(F32) ** 2)
            block = block.reshape(2, block.shape[0] // 2, self.half)
            mine = lax.dynamic_index_in_dim(block, self.core, 0, False)
            theirs = swap(lax.dynamic_index_in_dim(block, 1 - self.core, 0, False), "core")
            left = jnp.where(self.core == 0, mine, theirs)
            right = jnp.where(self.core == 0, theirs, mine)
            self.found = jnp.concatenate([left, right], 1)
            return block

    def step(x, dy, *arrays):
        weights, m, v = (arrays[i : i + 3] for i in (0, 3, 6))
        me = lax.axis_index("dp")
        core = me % 2
        bits = (me // 8 % 2, me // 4 % 2, me // 2 % 2)

        orders = [(0, 1, 2), (1, 2, 0), (2, 0, 1)]

        def scattered(a, b, turn):
            rows = a.shape[1] // 8
            if turn is not None:
                return Scattered(a, b, [(rows, orders[turn])], core, bits)
            third = rows // 3 // 16 * 16
            return Scattered(a, b, [(rows - 2 * third, orders[0]), (third, orders[1]), (third, orders[2])], core, bits)

        shards = [[w[number] for w in weights] for number in range(2)]
        gate_w0, up_w0 = gathered(shards[0][:2], 1)
        h0 = x[0]
        a0 = normed(h0)
        gate0, up0, hid0, down_w0, gate_w1 = hidden(a0, gate_w0, up_w0, [shards[0][2], shards[1][0]], [(0, 5, 9, 11), (0, 10, 16, 18)], 2)
        h1, up_w1 = lowered(hid0, down_w0, h0, [shards[1][1]], [(0, 4, 7, 7)], 3)
        a1, unnormed = jax.vjp(normed, h1)
        gate1, up1, hid1, down_w1 = hidden(a1, gate_w1, up_w1, [shards[1][2]], [(0, 6, 11, 14)], 4)
        full = [[gate_w0, up_w0, down_w0], [gate_w1, up_w1, down_w1]]

        by = dy[0]
        by_gate1, by_up1 = unhidden(by, full[1][2], gate1, up1)
        d1 = scattered(hid1, by, None)
        t = d1.other(by_gate1)
        by_gate, w = after((by_gate1, full[1][0]), t)
        by_a = dot(by_gate, w, (1, 1))
        t = d1.own(by_a)
        t = d1.halve(0, t)
        by_up, w = after((by_up1, full[1][1]), t)
        by_a = (by_a + dot(by_up, w, (1, 1))).astype(BF16)
        t = d1.halve(1, by_a)
        by = by + unnormed(after(by_a, t))[0]
        g1, u1 = scattered(a1, by_gate1, None), scattered(a1, by_up1, None)
        t = g1.other(by)
        t = d1.halve(2, t)
        t = u1.other(t)
        t = d1.finish(t)
        t = g1.own(t)
        t = g1.halve(0, t)
        t = u1.own(t)
        t = u1.halve(0, t)
        by = after(by, t)
        by_gate0, by_up0 = unhidden(by, full[0][2], gate0, up0)
        t = g1.halve(1, by_gate0)
        t = u1.halve(1, t)
        d0 = scattered(hid0, by, None)
        g0, u0 = scattered(a0, by_gate0, None), scattered(a0, by_up0, None)
        t = d0.other(t)
        t = g1.halve(2, t)
        t = u1.halve(2, t)
        t = g0.other(t)
        t = d0.own(t)
        t = d0.halve(0, t)
        t = u0.other(t)
        t = g1.finish(t)
        t = u1.finish(t)
        t = g0.own(t)
        t = g0.halve(0, t)
        t = d0.halve(1, t)
        t = u0.own(t)
        t = u0.halve(0, t)
        t = d0.halve(2, t)
        t = g0.halve(1, t)
        t = d0.finish(t)
        t = g0.halve(2, t)
        t = u0.halve(1, t)
        t = g0.finish(t)
        t = u0.halve(2, t)
        t = u0.finish(t)
        gate0_, gate1_, up0_, up1_, down0, down1 = g0, g1, u0, u1, d0, d1

        pairs = [[gate0_, gate1_], [up0_, up1_], [down0, down1]]
        squares = sum(one.squares for pair in pairs for one in pair)
        spread = jnp.where((lax.broadcasted_iota(jnp.int32, (8, 128), 0) == 0) & (lax.broadcasted_iota(jnp.int32, (8, 128), 1) == 0), squares, 0.0)
        total = jnp.sum(everywhere(n, spread))
        count = n * sum(w.size for w in weights)
        factor = jnp.minimum(1.0, 0.5 * lax.rsqrt(total / count + 1e-30))
        new = []
        for w, mm, vv, pair in zip(weights, m, v, pairs, strict=True):
            g = jnp.stack([one.found for one in pair]).astype(F32) * factor
            new.append(adamw(w.astype(F32), mm, vv, g))
        return tuple(one[which] for which in range(3) for one in new)

    states, cut = P(("rep", "dp"), None, None), P(None, "dp", None)
    return jax.shard_map(
        step,
        mesh=mesh,
        in_specs=(states, states) + (cut,) * 9,
        out_specs=(P("rep", "dp", None),) * 9,
        check_vma=False,
    )
```

```python
import jax
import jax.numpy as jnp
from jax import lax
from jax.experimental import pallas as pl
from jax.experimental.pallas import tpu as pltpu
from jax.sharding import PartitionSpec as P

F32, BF16 = jnp.float32, jnp.bfloat16


def normed(h):
    wide = h.astype(F32)
    scale = lax.rsqrt(jnp.mean(wide**2, -1, keepdims=True) + 1e-6)
    return (wide * scale).astype(BF16)


def adamw(w, m, v, g):
    m = 0.9 * m + 0.1 * g
    v = 0.95 * v + 0.05 * g * g
    step = m * lax.rsqrt(v + 1e-8) + 0.1 * w
    return (w - 0.02 * step).astype(BF16), m, v


def dot(a, b, contract):
    return lax.dot_general(a, b, ((contract[:1], contract[1:]), ((), ())), preferred_element_type=F32)


def everywhere(n, part):
    def kernel(part_ref, out_ref, slots, send_sem, recv_sem):
        me = lax.axis_index("dp")
        barrier = pltpu.get_barrier_semaphore()
        for k in range(1, n):
            pl.semaphore_signal(barrier, inc=1, device_id={"dp": lax.rem(me + k, n)}, device_id_type=pl.DeviceIdType.MESH)
        pl.semaphore_wait(barrier, n - 1)
        copies = []
        for k in range(1, n):
            copy = pltpu.make_async_remote_copy(
                src_ref=part_ref,
                dst_ref=slots.at[k],
                send_sem=send_sem.at[k],
                recv_sem=recv_sem.at[k],
                device_id={"dp": lax.rem(me + k, n)},
                device_id_type=pl.DeviceIdType.MESH,
            )
            copy.start()
            copies.append(copy)
        total = part_ref[...]
        for k, copy in enumerate(copies, 1):
            copy.wait()
            total = total + slots[k]
        out_ref[...] = total

    return pl.pallas_call(
        kernel,
        out_shape=jax.ShapeDtypeStruct((8, 128), F32),
        in_specs=[pl.BlockSpec(memory_space=pltpu.VMEM)],
        out_specs=pl.BlockSpec(memory_space=pltpu.VMEM),
        scratch_shapes=[pltpu.VMEM((n, 8, 128), F32), pltpu.SemaphoreType.DMA((n,)), pltpu.SemaphoreType.DMA((n,))],
        compiler_params=pltpu.CompilerParams(collective_id=0, has_side_effects=True),
    )(part)


def across(bits):
    owner = lax.axis_index("dp")
    for bit in (8, 4, 2, 1):
        if bits & bit:
            owner = owner + bit - 2 * bit * (owner // bit % 2)
    return owner


def thirds(cols):
    later = cols // 128 // 3 * 128
    return [(0, cols - 2 * later), (cols - 2 * later, later), (cols - later, later)]


class Gather:
    SENDS = [(0, 8), (0, 4), (0, 2), (8, 4), (4, 2), (2, 8), (12, 2), (6, 8), (10, 4)]
    HANDED = [0, 8, 4, 2, 12, 6, 10, 14]
    COPIES = 17

    def __init__(self, shard, full, send_sem, recv_sem, local_sem):
        rows, cols = shard.shape
        spans = thirds(cols)

        def block(bits, third=None):
            start = pl.multiple_of(across(bits) * rows, 16)
            if third is None:
                return full.at[pl.ds(start, rows), :]
            return full.at[pl.ds(start, rows), pl.ds(spans[third][0], spans[third][1])]

        def copy(k, bits, to, third=None):
            return pltpu.make_async_remote_copy(
                src_ref=shard if bits == 0 else block(bits, third),
                dst_ref=block(bits, third),
                send_sem=send_sem.at[k],
                recv_sem=recv_sem.at[k],
                device_id={"dp": across(to)},
                device_id_type=pl.DeviceIdType.MESH,
            )

        self.far = [copy(k, bits, to, k - 6 if k >= 6 else None) for k, (bits, to) in enumerate(self.SENDS)]
        self.near = [copy(9 + k, bits, 1) for k, bits in enumerate(self.HANDED)]
        self.local = pltpu.make_async_copy(shard, block(0), local_sem)

    def then(self, phase):
        pass

    def before(self, number):
        if number == 0:
            for copy in self.far[:3] + self.near[:1] + [self.local]:
                copy.start()
        elif number < 3:
            for k in range(3 * number - 3, 3 * number):
                self.far[k].wait_recv()
                self.far[k + 3].start()
                self.near[k + 1].start()
        else:
            for k in range(6, 9):
                self.far[k].wait_recv()
            self.near[7].start()

    def last(self):
        for copy in self.near:
            copy.wait_recv()
        for copy in self.far + self.near:
            copy.wait_send()
        self.local.wait()


def meet():
    barrier = pltpu.get_barrier_semaphore()
    for bit in (8, 4, 2, 1):
        pl.semaphore_signal(barrier, inc=1, device_id={"dp": across(bit)}, device_id_type=pl.DeviceIdType.MESH)
    pl.semaphore_wait(barrier, 4)


class Scatter:
    COPIES = 17
    PAIRS = [14, 12, 6, 10, 8, 4, 2, 0]
    LINKS = [[2, 8, 4], [4, 2, 8], [8, 4, 2]]
    SUMS = [[14], [12, 6, 10], [8, 4, 2]]

    @staticmethod
    def scratch(rows, cols):
        one = lambda n, t=BF16: pltpu.VMEM((n, rows, cols), t)
        return [one(8), one(8, F32), one(1), one(3), one(3), one(1), one(3), one(3)] + [
            pltpu.SemaphoreType.DMA((17,)), pltpu.SemaphoreType.DMA((17,)), pltpu.SemaphoreType.DMA((8,))
        ]

    def __init__(self, leave, stay, out, squares, pair, held, *more):
        *buffers, send_sem, recv_sem, local_sem = more
        self.out, self.squares, self.pair, self.held = out, squares, pair, held
        self.going, self.came = buffers[:3], buffers[3:]
        _, self.rows, cols = pair.shape
        self.spans = thirds(cols)

        def copy(k, src, dst, to):
            return pltpu.make_async_remote_copy(
                src_ref=src,
                dst_ref=dst,
                send_sem=send_sem.at[k],
                recv_sem=recv_sem.at[k],
                device_id={"dp": across(to)},
                device_id_type=pl.DeviceIdType.MESH,
            )

        self.near = [copy(k, leave.at[across(m) // 2], pair.at[m // 2], 1) for k, m in enumerate(self.PAIRS)]
        self.loads = [pltpu.make_async_copy(stay.at[across(m) // 2], held.at[m // 2], local_sem.at[k]) for k, m in enumerate(self.PAIRS)]
        self.far = []
        for stage, links in enumerate(self.LINKS):
            made = []
            for i, link in enumerate(links):
                src, dst = self.going[stage].at[i if stage else 0], self.came[stage].at[i if stage else 0]
                if stage == 0:
                    columns = pl.ds(self.spans[i][0], self.spans[i][1])
                    src, dst = src.at[:, columns], dst.at[:, columns]
                made.append(copy(8 + 3 * stage + i, src, dst, link))
            self.far.append(made)

    def ready(self, m):
        k = self.PAIRS.index(m)
        self.near[k].wait_recv()
        self.loads[k].wait()

    def before(self, phase):
        if phase == 0:
            for one in self.near + self.loads:
                one.start()
            return
        stage = phase - 1
        for m in self.SUMS[stage]:
            self.ready(m)
        if stage:
            for copy in self.far[stage - 1]:
                copy.wait_recv()
        for i, m in enumerate(self.SUMS[stage]):

            def add(r, _, i=i, m=m):
                some = pl.ds(pl.multiple_of(r * 16, 16), 16)
                for t, (start, size) in enumerate(self.spans):
                    columns = pl.ds(start, size)
                    value = self.held[m // 2, some, columns] + self.pair[m // 2, some, columns].astype(F32)
                    if stage == 1 and t == i:
                        value = value + self.came[0][0, some, columns].astype(F32)
                    if stage == 2:
                        value = value + self.came[1][i, some, columns].astype(F32)
                    self.going[stage][i, some, columns] = value.astype(BF16)
                return 0

            lax.fori_loop(0, self.rows // 16, add, 0)

    def then(self, phase):
        if phase:
            for copy in self.far[phase - 1]:
                copy.start()

    def last(self):
        self.ready(0)
        for copy in self.far[2]:
            copy.wait_recv()

        def add(r, total):
            some = pl.ds(pl.multiple_of(r * 16, 16), 16)
            value = self.held[0, some, :] + self.pair[0, some, :].astype(F32)
            for i in range(3):
                value = value + self.came[2][i, some, :].astype(F32)
            value = value.astype(BF16)
            self.out[some, :] = value
            value = value.astype(F32)
            value = value * value
            return sum((value[:, at : at + 128] for at in range(0, value.shape[1], 128)), total)

        total = lax.fori_loop(0, self.rows // 16, add, jnp.zeros((16, 128), F32))
        self.squares[...] = total[:8] + total[8:]
        for copy in self.near + self.far[0] + self.far[1] + self.far[2]:
            copy.wait_send()


def hosting(body, steps, operands, in_specs, out_shape, out_specs, tasks, identity, flops, moved, own_scratch=()):
    given, made = len(operands), len(out_shape)
    anywhere = pl.BlockSpec(memory_space=pl.ANY)
    task_ins, task_outs, task_out_specs, scratch, shape_of = [], [], [], [], []
    for arrays, *_ in tasks:
        if len(arrays) == 1:
            _, rows, cols = arrays[0].shape
            task_outs.append([jax.ShapeDtypeStruct((16 * rows, cols), BF16)])
            task_out_specs.append(anywhere)
            more = [pltpu.SemaphoreType.DMA((Gather.COPIES,)), pltpu.SemaphoreType.DMA((Gather.COPIES,)), pltpu.SemaphoreType.DMA(())]
        else:
            _, rows, cols = arrays[0].shape
            task_outs.append([jax.ShapeDtypeStruct((rows, cols), BF16), jax.ShapeDtypeStruct((8, 128), F32)])
            task_out_specs += [pl.BlockSpec((rows, cols), lambda i: (0, 0)), pl.BlockSpec((8, 128), lambda i: (0, 0))]
            more = Scatter.scratch(rows, cols)
        shape_of.append((len(arrays), len(more)))
        task_ins += arrays
        scratch += more
    scratch += list(own_scratch)

    def kernel(*refs):
        refs = list(refs)
        take = lambda k: [refs.pop(0) for _ in range(k)]
        ins = take(given)
        task_in = [take(n) for n, _ in shape_of]
        outs = take(made)
        task_out = [take(len(one)) for one in task_outs]
        running = []
        for (n, k), mine, out, (_, _, *layer) in zip(shape_of, task_in, task_out, tasks, strict=True):
            if n == 1:
                mine = [mine[0].at[layer[0]]]
            running.append((Gather if n == 1 else Scatter)(*mine, *out, *take(k)))
        step = pl.program_id(0)

        def due(now, action):
            wait = 1 if body is None and action == "then" else 0
            todo = sorted((phase, i) for i, (_, when, *_) in enumerate(tasks) for phase in range(4) if when[phase] + wait == now)
            if todo:

                @pl.when(step == now)
                def _():
                    if now == 0 and action == "before":
                        meet()
                    for phase, i in todo:
                        getattr(running[i], action)(phase)

        for now in range(steps):
            due(now, "before")
        if body is not None:
            body(*ins, *outs, *refs)
        for now in range(steps):
            due(now, "then")

        @pl.when(step == steps - 1)
        def _():
            for one in running:
                one.last()

    return pl.pallas_call(
        kernel,
        grid=(steps,),
        out_shape=list(out_shape) + sum(task_outs, []),
        in_specs=list(in_specs) + [anywhere] * len(task_ins),
        out_specs=list(out_specs) + task_out_specs,
        scratch_shapes=scratch,
        compiler_params=pltpu.CompilerParams(
            collective_id=identity, has_side_effects=True, dimension_semantics=("arbitrary",), vmem_limit_bytes=67043328
        ),
        cost_estimate=pl.CostEstimate(flops=flops, bytes_accessed=moved, transcendentals=0),
    )(*operands, *task_ins)


def plain(body, steps, operands, in_specs, out_shape, out_specs, flops, moved):
    return pl.pallas_call(
        body,
        grid=(steps,),
        out_shape=out_shape,
        in_specs=in_specs,
        out_specs=out_specs,
        compiler_params=pltpu.CompilerParams(dimension_semantics=("arbitrary",), vmem_limit_bytes=67043328),
        cost_estimate=pl.CostEstimate(flops=flops, bytes_accessed=moved, transcendentals=0),
    )(*operands)


def by_weight(a, b, tasks=(), identity=None):
    tokens, m = a.shape
    n = b.shape[1]
    rows = m // 16

    def parted(acc, leave_ref, stay_ref):
        core = lax.axis_index("dp") % 2
        first, second = acc[:, 0], acc[:, 1]
        leave_ref[...] = jnp.where(core == 0, second, first).astype(BF16)
        stay_ref[...] = jnp.where(core == 0, first, second)

    if m < n:
        wide, steps = 512, n // 512

        def body(a_ref, b_ref, leave_ref, stay_ref):
            acc = lax.dot_general(a_ref[...], b_ref[...], (((0,), (0,)), ((), ())), preferred_element_type=F32)
            parted(acc.reshape(8, 2, rows, wide), leave_ref, stay_ref)

        specs = [pl.BlockSpec((tokens, m), lambda j: (0, 0)), pl.BlockSpec((tokens, wide), lambda j: (0, j))]
        out = pl.BlockSpec((8, rows, wide), lambda j: (0, 0, j))
    else:
        steps = 8

        def body(a_ref, b_ref, leave_ref, stay_ref):
            acc = lax.dot_general(a_ref[...], b_ref[...], (((0,), (0,)), ((), ())), preferred_element_type=F32)
            parted(acc.reshape(1, 2, rows, n), leave_ref, stay_ref)

        specs = [pl.BlockSpec((tokens, m // 8), lambda j: (0, j)), pl.BlockSpec((tokens, n), lambda j: (0, 0))]
        out = pl.BlockSpec((1, rows, n), lambda j: (j, 0, 0))
    shapes = [jax.ShapeDtypeStruct((8, rows, n), t) for t in (BF16, F32)]
    flops = 2 * tokens * m * n
    if not tasks:
        return plain(body, steps, [a, b], specs, shapes, [out, out], flops, 70 * 2**20)
    return hosting(body, steps, [a, b], specs, shapes, [out, out], tasks, identity, flops, 70 * 2**20)


def gathered(h, tasks, identity):
    tokens, d = h.shape
    tall = 256

    def body(h_ref, a_ref):
        a_ref[...] = normed(h_ref[...])

    row = pl.BlockSpec((tall, d), lambda i: (i, 0))
    like = [jax.ShapeDtypeStruct((tokens, d), BF16)]
    return hosting(body, tokens // tall, [h], [row], like, [row], tasks, identity, 10**9, 10**8)


def hidden(a, w_gate, w_up, tasks, identity):
    tokens, d = a.shape
    ff = w_gate.shape[1]
    wide = 256

    def body(a_ref, gate_w, up_w, gate_ref, up_ref, hid_ref):
        gate = jnp.dot(a_ref[...], gate_w[...], preferred_element_type=F32)
        up = jnp.dot(a_ref[...], up_w[...], preferred_element_type=F32)
        gate_ref[...] = gate
        up_ref[...] = up
        hid_ref[...] = (gate * jax.nn.sigmoid(gate) * up).astype(BF16)

    weight, out = pl.BlockSpec((d, wide), lambda j: (0, j)), pl.BlockSpec((tokens, wide), lambda j: (0, j))
    like = [jax.ShapeDtypeStruct((tokens, ff), t) for t in (F32, F32, BF16)]
    specs = [pl.BlockSpec((tokens, d), lambda j: (0, 0)), weight, weight]
    return hosting(body, ff // wide, [a, w_gate, w_up], specs, like, [out] * 3, tasks, identity, 4 * tokens * d * ff, 150 * 2**20)


def lowered(hid, w_down, h, tasks, identity):
    tokens, ff = hid.shape
    d = w_down.shape[1]
    tall = 256

    def body(hid_ref, w_ref, h_ref, out_ref, a_ref):
        h = h_ref[...] + jnp.dot(hid_ref[...], w_ref[...], preferred_element_type=F32).astype(BF16)
        out_ref[...] = h
        a_ref[...] = normed(h)

    row = pl.BlockSpec((tall, d), lambda i: (i, 0))
    specs = [pl.BlockSpec((tall, ff), lambda i: (i, 0)), pl.BlockSpec((ff, d), lambda i: (0, 0)), row]
    like = [jax.ShapeDtypeStruct((tokens, d), BF16)] * 2
    return hosting(body, tokens // tall, [hid, w_down, h], specs, like, [row] * 2, tasks, identity, 2 * tokens * d * ff, 60 * 2**20)


def unhidden(by, w_down, gate, up, tasks, identity):
    tokens, d = by.shape
    ff = w_down.shape[0]
    wide = 256

    def body(by_ref, w_ref, gate_ref, up_ref, by_gate, by_up):
        by_hid = lax.dot_general(by_ref[...], w_ref[...], (((1,), (1,)), ((), ())), preferred_element_type=F32).astype(BF16).astype(F32)
        gate = gate_ref[...]
        s = jax.nn.sigmoid(gate)
        by_up[...] = (by_hid * (gate * s)).astype(BF16)
        by_gate[...] = (by_hid * up_ref[...] * (s * (1 + gate * (1 - s)))).astype(BF16)

    block = pl.BlockSpec((tokens, wide), lambda j: (0, j))
    like = [jax.ShapeDtypeStruct((tokens, ff), BF16)] * 2
    specs = [pl.BlockSpec((tokens, d), lambda j: (0, 0)), pl.BlockSpec((wide, d), lambda j: (j, 0)), block, block]
    return hosting(body, ff // wide, [by, w_down, gate, up], specs, like, [block] * 2, tasks, identity, 2 * tokens * d * ff, 140 * 2**20)


def by_normed(by_gate, by_up, w_gate, w_up, tasks, identity):
    tokens, ff = by_gate.shape
    d = w_gate.shape[0]
    wide = 256
    steps = ff // wide

    def body(by_gate_ref, by_up_ref, gate_w, up_w, out_ref, total):
        step = pl.program_id(0)
        term = lax.dot_general(by_gate_ref[...], gate_w[...], (((1,), (1,)), ((), ())), preferred_element_type=F32)
        term = term + lax.dot_general(by_up_ref[...], up_w[...], (((1,), (1,)), ((), ())), preferred_element_type=F32)

        @pl.when(step == 0)
        def _():
            total[...] = term

        @pl.when(step > 0)
        def _():
            total[...] += term

        @pl.when(step == steps - 1)
        def _():
            out_ref[...] = total[...].astype(BF16)

    block, weight = pl.BlockSpec((tokens, wide), lambda j: (0, j)), pl.BlockSpec((d, wide), lambda j: (0, j))
    like = [jax.ShapeDtypeStruct((tokens, d), BF16)]
    out = pl.BlockSpec((tokens, d), lambda j: (0, 0))
    flops = 4 * tokens * d * ff
    operands, own = [by_gate, by_up, w_gate, w_up], [pltpu.VMEM((tokens, d), F32)]
    return hosting(body, steps, operands, [block, block, weight, weight], like, [out], tasks, identity, flops, 80 * 2**20, own)


def scattered(parts, identity):
    return hosting(None, 9, [], [], [], [], [(parts, (0, 2, 4, 6))], identity, 10**9, 10**8)


def solution(mesh):
    n = mesh.shape["dp"]
    def step(x, dy, *arrays):
        weights, m, v = (arrays[i : i + 3] for i in (0, 3, 6))
        gate, up, down = ([w] for w in weights)
        h0 = x[0]
        a0, gate_w0, up_w0 = gathered(h0, [(gate, (0, 1, 3, 5), 0), (up, (0, 2, 4, 6), 0)], 1)
        tasks = [(down, (0, 5, 9, 11), 0), (gate, (0, 10, 16, 18), 1)]
        gate0, up0, hid0, down_w0, gate_w1 = hidden(a0, gate_w0, up_w0, tasks, 2)
        h1, a1, up_w1 = lowered(hid0, down_w0, h0, [(up, (0, 4, 7, 7), 1)], 3)
        gate1, up1, hid1, down_w1 = hidden(a1, gate_w1, up_w1, [(down, (0, 6, 11, 14), 1)], 4)

        by = dy[0]
        down1 = list(by_weight(hid1, by))
        by_gate1, by_up1, *g_down1 = unhidden(by, down_w1, gate1, up1, [(down1, (0, 1, 5, 11))], 5)
        in_gate1 = list(by_weight(a1, by_gate1))
        by_a, *g_gate1 = by_normed(by_gate1, by_up1, gate_w1, up_w1, [(in_gate1, (0, 1, 5, 11))], 6)
        by = by + jax.vjp(normed, h1)[1](by_a)[0]
        in_up1 = list(by_weight(a1, by_up1))
        by_gate0, by_up0, *g_up1 = unhidden(by, down_w0, gate0, up0, [(in_up1, (0, 1, 5, 11))], 7)
        down0 = list(by_weight(hid0, by))
        *in_gate0, g_down0, s_down0 = by_weight(a0, by_gate0, [(down0, (0, 1, 4, 8))], 8)
        *in_up0, g_gate0, s_gate0 = by_weight(a0, by_up0, [(in_gate0, (0, 1, 4, 8))], 9)
        g_up0 = scattered(in_up0, 10)

        both = [[(g_gate0, s_gate0), g_gate1], [g_up0, g_up1], [(g_down0, s_down0), g_down1]]
        pairs = [[one[0] for one in pair] for pair in both]
        total = jnp.sum(everywhere(n, sum(one[1] for pair in both for one in pair)))
        count = n * sum(w.size for w in weights)
        factor = jnp.minimum(1.0, 0.5 * lax.rsqrt(total / count + 1e-30))
        new = []
        for w, mm, vv, pair in zip(weights, m, v, pairs, strict=True):
            g = jnp.stack(pair).astype(F32) * factor
            new.append(adamw(w.astype(F32), mm, vv, g))
        return tuple(one[which] for which in range(3) for one in new)

    states, cut = P(("rep", "dp"), None, None), P(None, "dp", None)
    return jax.shard_map(
        step,
        mesh=mesh,
        in_specs=(states, states) + (cut,) * 9,
        out_specs=(P("rep", "dp", None),) * 9,
        check_vma=False,
    )
```

```python
import jax
import jax.numpy as jnp
from jax import lax
from jax.experimental import pallas as pl
from jax.experimental.pallas import tpu as pltpu
from jax.sharding import PartitionSpec as P

F32, BF16 = jnp.float32, jnp.bfloat16


def normed(h):
    wide = h.astype(F32)
    scale = lax.rsqrt(jnp.mean(wide**2, -1, keepdims=True) + 1e-6)
    return (wide * scale).astype(BF16)


def adamw(w, m, v, g):
    m = 0.9 * m + 0.1 * g
    v = 0.95 * v + 0.05 * g * g
    step = m * lax.rsqrt(v + 1e-8) + 0.1 * w
    return (w - 0.02 * step).astype(BF16), m, v


def dot(a, b, contract):
    return lax.dot_general(a, b, ((contract[:1], contract[1:]), ((), ())), preferred_element_type=F32)


def everywhere(n, part):
    def kernel(part_ref, out_ref, slots, send_sem, recv_sem):
        me = lax.axis_index("dp")
        barrier = pltpu.get_barrier_semaphore()
        for k in range(1, n):
            pl.semaphore_signal(barrier, inc=1, device_id={"dp": lax.rem(me + k, n)}, device_id_type=pl.DeviceIdType.MESH)
        pl.semaphore_wait(barrier, n - 1)
        copies = []
        for k in range(1, n):
            copy = pltpu.make_async_remote_copy(
                src_ref=part_ref,
                dst_ref=slots.at[k],
                send_sem=send_sem.at[k],
                recv_sem=recv_sem.at[k],
                device_id={"dp": lax.rem(me + k, n)},
                device_id_type=pl.DeviceIdType.MESH,
            )
            copy.start()
            copies.append(copy)
        total = part_ref[...]
        for k, copy in enumerate(copies, 1):
            copy.wait()
            total = total + slots[k]
        out_ref[...] = total

    return pl.pallas_call(
        kernel,
        out_shape=jax.ShapeDtypeStruct((8, 128), F32),
        in_specs=[pl.BlockSpec(memory_space=pltpu.VMEM)],
        out_specs=pl.BlockSpec(memory_space=pltpu.VMEM),
        scratch_shapes=[pltpu.VMEM((n, 8, 128), F32), pltpu.SemaphoreType.DMA((n,)), pltpu.SemaphoreType.DMA((n,))],
        compiler_params=pltpu.CompilerParams(collective_id=0, has_side_effects=True),
    )(part)


def across(bits):
    owner = lax.axis_index("dp")
    for bit in (8, 4, 2, 1):
        if bits & bit:
            owner = owner + bit - 2 * bit * (owner // bit % 2)
    return owner


def thirds(cols):
    later = cols // 128 // 3 * 128
    return [(0, cols - 2 * later), (cols - 2 * later, later), (cols - later, later)]


class Gather:
    SENDS = [(0, 8), (0, 4), (0, 2), (8, 4), (4, 2), (2, 8), (12, 2), (6, 8), (10, 4)]
    HANDED = [0, 8, 4, 2, 12, 6, 10, 14]
    COPIES = 17

    def __init__(self, shard, full, send_sem, recv_sem, local_sem):
        rows, cols = shard.shape
        spans = thirds(cols)

        def block(bits, third=None):
            start = pl.multiple_of(across(bits) * rows, 16)
            if third is None:
                return full.at[pl.ds(start, rows), :]
            return full.at[pl.ds(start, rows), pl.ds(spans[third][0], spans[third][1])]

        def copy(k, bits, to, third=None):
            return pltpu.make_async_remote_copy(
                src_ref=shard if bits == 0 else block(bits, third),
                dst_ref=block(bits, third),
                send_sem=send_sem.at[k],
                recv_sem=recv_sem.at[k],
                device_id={"dp": across(to)},
                device_id_type=pl.DeviceIdType.MESH,
            )

        self.far = [copy(k, bits, to, k - 6 if k >= 6 else None) for k, (bits, to) in enumerate(self.SENDS)]
        self.near = [copy(9 + k, bits, 1) for k, bits in enumerate(self.HANDED)]
        self.local = pltpu.make_async_copy(shard, block(0), local_sem)

    def start(self, number):
        if number == 0:
            for copy in self.far[:3] + self.near[:1] + [self.local]:
                copy.start()
        elif number < 3:
            for k in range(3 * number - 3, 3 * number):
                self.far[k].wait_recv()
                self.far[k + 3].start()
                self.near[k + 1].start()
        else:
            for k in range(6, 9):
                self.far[k].wait_recv()
            self.near[7].start()

    def last(self):
        for copy in self.near:
            copy.wait_recv()
        for copy in self.far + self.near:
            copy.wait_send()
        self.local.wait()


def meet():
    barrier = pltpu.get_barrier_semaphore()
    for bit in (8, 4, 2, 1):
        pl.semaphore_signal(barrier, inc=1, device_id={"dp": across(bit)}, device_id_type=pl.DeviceIdType.MESH)
    pl.semaphore_wait(barrier, 4)


class Scatter:
    COPIES = 17
    PAIRS = [14, 12, 6, 10, 8, 4, 2, 0]
    LINKS = [[2, 8, 4], [4, 2, 8], [8, 4, 2]]
    SUMS = [[14], [12, 6, 10], [8, 4, 2]]

    @staticmethod
    def scratch(rows, cols):
        one = lambda n, t=BF16: pltpu.VMEM((n, rows, cols), t)
        return [one(8), one(8, F32), one(1), one(3), one(3), one(1), one(3), one(3)] + [
            pltpu.SemaphoreType.DMA((17,)), pltpu.SemaphoreType.DMA((17,)), pltpu.SemaphoreType.DMA((8,))
        ]

    def __init__(self, leave, stay, out, squares, pair, held, *more):
        *buffers, send_sem, recv_sem, local_sem = more
        self.out, self.squares, self.pair, self.held = out, squares, pair, held
        self.going, self.came = buffers[:3], buffers[3:]
        _, self.rows, cols = pair.shape
        self.spans = thirds(cols)

        def copy(k, src, dst, to):
            return pltpu.make_async_remote_copy(
                src_ref=src,
                dst_ref=dst,
                send_sem=send_sem.at[k],
                recv_sem=recv_sem.at[k],
                device_id={"dp": across(to)},
                device_id_type=pl.DeviceIdType.MESH,
            )

        self.near = [copy(k, leave.at[across(m) // 2], pair.at[m // 2], 1) for k, m in enumerate(self.PAIRS)]
        self.loads = [pltpu.make_async_copy(stay.at[across(m) // 2], held.at[m // 2], local_sem.at[k]) for k, m in enumerate(self.PAIRS)]
        self.far = []
        for stage, links in enumerate(self.LINKS):
            made = []
            for i, link in enumerate(links):
                src, dst = self.going[stage].at[i if stage else 0], self.came[stage].at[i if stage else 0]
                if stage == 0:
                    columns = pl.ds(self.spans[i][0], self.spans[i][1])
                    src, dst = src.at[:, columns], dst.at[:, columns]
                made.append(copy(8 + 3 * stage + i, src, dst, link))
            self.far.append(made)

    def ready(self, m):
        k = self.PAIRS.index(m)
        self.near[k].wait_recv()
        self.loads[k].wait()

    def start(self, phase):
        if phase == 0:
            for one in self.near + self.loads:
                one.start()

    def sum(self, phase):
        stage = phase - 1
        for m in self.SUMS[stage]:
            self.ready(m)
        if stage:
            for copy in self.far[stage - 1]:
                copy.wait_recv()
        for i, m in enumerate(self.SUMS[stage]):

            def add(r, _, i=i, m=m):
                some = pl.ds(pl.multiple_of(r * 16, 16), 16)
                for t, (start, size) in enumerate(self.spans):
                    columns = pl.ds(start, size)
                    value = self.held[m // 2, some, columns] + self.pair[m // 2, some, columns].astype(F32)
                    if stage == 1 and t == i:
                        value = value + self.came[0][0, some, columns].astype(F32)
                    if stage == 2:
                        value = value + self.came[1][i, some, columns].astype(F32)
                    self.going[stage][i, some, columns] = value.astype(BF16)
                return 0

            lax.fori_loop(0, self.rows // 16, add, 0)

    def send(self, phase):
        for copy in self.far[phase - 1]:
            copy.start()

    def last(self):
        self.ready(0)
        for copy in self.far[2]:
            copy.wait_recv()

        def add(r, total):
            some = pl.ds(pl.multiple_of(r * 16, 16), 16)
            value = self.held[0, some, :] + self.pair[0, some, :].astype(F32)
            for i in range(3):
                value = value + self.came[2][i, some, :].astype(F32)
            value = value.astype(BF16)
            self.out[some, :] = value
            value = value.astype(F32)
            value = value * value
            return sum((value[:, at : at + 128] for at in range(0, value.shape[1], 128)), total)

        total = lax.fori_loop(0, self.rows // 16, add, jnp.zeros((16, 128), F32))
        self.squares[...] = total[:8] + total[8:]
        for copy in self.near + self.far[0] + self.far[1] + self.far[2]:
            copy.wait_send()


def hosting(body, steps, operands, in_specs, out_shape, out_specs, tasks, identity, flops, moved, own_scratch=(), idle=0):
    given, made = len(operands), len(out_shape)
    anywhere = pl.BlockSpec(memory_space=pl.ANY)
    task_ins, task_outs, task_out_specs, scratch, shape_of = [], [], [], [], []
    for arrays, *_ in tasks:
        if len(arrays) == 1:
            _, rows, cols = arrays[0].shape
            task_outs.append([jax.ShapeDtypeStruct((16 * rows, cols), BF16)])
            task_out_specs.append(anywhere)
            more = [pltpu.SemaphoreType.DMA((Gather.COPIES,)), pltpu.SemaphoreType.DMA((Gather.COPIES,)), pltpu.SemaphoreType.DMA(())]
        else:
            _, rows, cols = arrays[0].shape
            task_outs.append([jax.ShapeDtypeStruct((rows, cols), BF16), jax.ShapeDtypeStruct((8, 128), F32)])
            task_out_specs += [pl.BlockSpec((rows, cols), lambda i: (0, 0)), pl.BlockSpec((8, 128), lambda i: (0, 0))]
            more = Scatter.scratch(rows, cols)
        shape_of.append((len(arrays), len(more)))
        task_ins += arrays
        scratch += more
    scratch += list(own_scratch)

    def kernel(*refs):
        refs = list(refs)
        take = lambda k: [refs.pop(0) for _ in range(k)]
        ins = take(given)
        task_in = [take(n) for n, _ in shape_of]
        outs = take(made)
        task_out = [take(len(one)) for one in task_outs]
        running = []
        for (n, k), mine, out, (_, _, *layer) in zip(shape_of, task_in, task_out, tasks, strict=True):
            if n == 1:
                mine = [mine[0].at[layer[0]]]
            running.append((Gather if n == 1 else Scatter)(*mine, *out, *take(k)))
        step = pl.program_id(0)

        def due(now, early):
            todo = []
            for i, ((arrays, when, *_), one) in enumerate(zip(tasks, running, strict=True)):
                for phase in range(4):
                    if len(arrays) == 1 or phase == 0:
                        todo += [(phase, i, one.start)] if early and when[phase] == now else []
                    elif early:
                        todo += [(phase, i, one.send)] if when[phase] + 1 == now else []
                    else:
                        todo += [(phase, i, one.sum)] if when[phase] == now else []
            if todo:

                @pl.when(step == now)
                def _():
                    if now == 0 and early:
                        meet()
                    for phase, _, action in sorted(todo, key=lambda one: one[:2]):
                        action(phase)

        for now in range(steps):
            due(now, True)
        if body is not None:
            if idle:
                pl.when(step < steps - idle)(lambda: body(*ins, *outs, *refs))
            else:
                body(*ins, *outs, *refs)
        for now in range(steps):
            due(now, False)

        @pl.when(step == steps - 1)
        def _():
            for one in running:
                one.last()

    return pl.pallas_call(
        kernel,
        grid=(steps,),
        out_shape=list(out_shape) + sum(task_outs, []),
        in_specs=list(in_specs) + [anywhere] * len(task_ins),
        out_specs=list(out_specs) + task_out_specs,
        scratch_shapes=scratch,
        compiler_params=pltpu.CompilerParams(
            collective_id=identity, has_side_effects=True, dimension_semantics=("arbitrary",), vmem_limit_bytes=67043328
        ),
        cost_estimate=pl.CostEstimate(flops=flops, bytes_accessed=moved, transcendentals=0),
    )(*operands, *task_ins)


def plain(body, steps, operands, in_specs, out_shape, out_specs, flops, moved):
    return pl.pallas_call(
        body,
        grid=(steps,),
        out_shape=out_shape,
        in_specs=in_specs,
        out_specs=out_specs,
        compiler_params=pltpu.CompilerParams(dimension_semantics=("arbitrary",), vmem_limit_bytes=67043328),
        cost_estimate=pl.CostEstimate(flops=flops, bytes_accessed=moved, transcendentals=0),
    )(*operands)


def by_weight(a, b, tasks=(), identity=None):
    tokens, m = a.shape
    n = b.shape[1]
    rows = m // 16

    def parted(acc, leave_ref, stay_ref):
        core = lax.axis_index("dp") % 2
        first, second = acc[:, 0], acc[:, 1]
        leave_ref[...] = jnp.where(core == 0, second, first).astype(BF16)
        stay_ref[...] = jnp.where(core == 0, first, second)

    idle = 2 if tasks else 0
    wide, real = 512, n // 512 if m < n else 8

    def at(j):
        return j - j // real * (j - real + 1)

    if m < n:

        def body(a_ref, b_ref, leave_ref, stay_ref):
            acc = lax.dot_general(a_ref[...], b_ref[...], (((0,), (0,)), ((), ())), preferred_element_type=F32)
            parted(acc.reshape(8, 2, rows, wide), leave_ref, stay_ref)

        specs = [pl.BlockSpec((tokens, m), lambda j: (0, 0)), pl.BlockSpec((tokens, wide), lambda j: (0, at(j)))]
        out = pl.BlockSpec((8, rows, wide), lambda j: (0, 0, at(j)))
    else:

        def body(a_ref, b_ref, leave_ref, stay_ref):
            acc = lax.dot_general(a_ref[...], b_ref[...], (((0,), (0,)), ((), ())), preferred_element_type=F32)
            parted(acc.reshape(1, 2, rows, n), leave_ref, stay_ref)

        specs = [pl.BlockSpec((tokens, m // 8), lambda j: (0, at(j))), pl.BlockSpec((tokens, n), lambda j: (0, 0))]
        out = pl.BlockSpec((1, rows, n), lambda j: (at(j), 0, 0))
    shapes = [jax.ShapeDtypeStruct((8, rows, n), t) for t in (BF16, F32)]
    flops = 2 * tokens * m * n
    if not tasks:
        return plain(body, real, [a, b], specs, shapes, [out, out], flops, 70 * 2**20)
    return hosting(body, real + idle, [a, b], specs, shapes, [out, out], tasks, identity, flops, 70 * 2**20, idle=idle)


def gathered(h, tasks, identity):
    tokens, d = h.shape
    tall = 256

    def body(h_ref, a_ref):
        a_ref[...] = normed(h_ref[...])

    row = pl.BlockSpec((tall, d), lambda i: (i, 0))
    like = [jax.ShapeDtypeStruct((tokens, d), BF16)]
    return hosting(body, tokens // tall, [h], [row], like, [row], tasks, identity, 10**9, 10**8)


def hidden(a, w_gate, w_up, tasks, identity, idle=0):
    tokens, d = a.shape
    ff = w_gate.shape[1]
    wide = 256
    real = ff // wide

    def at(j):
        return j - j // real * (j - real + 1)

    def body(a_ref, gate_w, up_w, gate_ref, up_ref, hid_ref):
        gate = jnp.dot(a_ref[...], gate_w[...], preferred_element_type=F32)
        up = jnp.dot(a_ref[...], up_w[...], preferred_element_type=F32)
        gate_ref[...] = gate
        up_ref[...] = up
        hid_ref[...] = (gate * jax.nn.sigmoid(gate) * up).astype(BF16)

    weight, out = pl.BlockSpec((d, wide), lambda j: (0, at(j))), pl.BlockSpec((tokens, wide), lambda j: (0, at(j)))
    like = [jax.ShapeDtypeStruct((tokens, ff), t) for t in (F32, F32, BF16)]
    specs = [pl.BlockSpec((tokens, d), lambda j: (0, 0)), weight, weight]
    return hosting(body, real + idle, [a, w_gate, w_up], specs, like, [out] * 3, tasks, identity, 4 * tokens * d * ff, 150 * 2**20, idle=idle)


def lowered(hid, w_down, h, tasks, identity):
    tokens, ff = hid.shape
    d = w_down.shape[1]
    tall, idle = 256, 2
    real = tokens // tall

    def at(i):
        return i - i // real * (i - real + 1)

    def body(hid_ref, w_ref, h_ref, out_ref, a_ref, held, sem):
        @pl.when(pl.program_id(0) == 0)
        def _():
            copy = pltpu.make_async_copy(w_ref, held, sem)
            copy.start()
            copy.wait()

        h = h_ref[...] + jnp.dot(hid_ref[...], held[...], preferred_element_type=F32).astype(BF16)
        out_ref[...] = h
        a_ref[...] = normed(h)

    row = pl.BlockSpec((tall, d), lambda i: (at(i), 0))
    specs = [pl.BlockSpec((tall, ff), lambda i: (at(i), 0)), pl.BlockSpec(memory_space=pl.ANY), row]
    like = [jax.ShapeDtypeStruct((tokens, d), BF16)] * 2
    return hosting(body, real + idle, [hid, w_down, h], specs, like, [row] * 2, tasks, identity, 2 * tokens * d * ff, 60 * 2**20, [pltpu.VMEM((ff, d), BF16), pltpu.SemaphoreType.DMA(())], idle)


def unhidden(by, w_down, gate, up, tasks, identity):
    tokens, d = by.shape
    ff = w_down.shape[0]
    wide = 256

    def body(by_ref, w_ref, gate_ref, up_ref, by_gate, by_up):
        by_hid = lax.dot_general(by_ref[...], w_ref[...], (((1,), (1,)), ((), ())), preferred_element_type=F32).astype(BF16).astype(F32)
        gate = gate_ref[...]
        s = jax.nn.sigmoid(gate)
        by_up[...] = (by_hid * (gate * s)).astype(BF16)
        by_gate[...] = (by_hid * up_ref[...] * (s * (1 + gate * (1 - s)))).astype(BF16)

    block = pl.BlockSpec((tokens, wide), lambda j: (0, j))
    like = [jax.ShapeDtypeStruct((tokens, ff), BF16)] * 2
    specs = [pl.BlockSpec((tokens, d), lambda j: (0, 0)), pl.BlockSpec((wide, d), lambda j: (j, 0)), block, block]
    return hosting(body, ff // wide, [by, w_down, gate, up], specs, like, [block] * 2, tasks, identity, 2 * tokens * d * ff, 140 * 2**20)


def by_normed(by_gate, by_up, w_gate, w_up, tasks, identity):
    tokens, ff = by_gate.shape
    d = w_gate.shape[0]
    wide = 256
    steps = ff // wide

    def body(by_gate_ref, by_up_ref, gate_w, up_w, out_ref, total):
        step = pl.program_id(0)
        for start in range(0, tokens, 512):
            some = pl.ds(start, 512)
            term = lax.dot_general(by_gate_ref[some, :], gate_w[...], (((1,), (1,)), ((), ())), preferred_element_type=F32)
            term = term + lax.dot_general(by_up_ref[some, :], up_w[...], (((1,), (1,)), ((), ())), preferred_element_type=F32)
            total[some, :] = jnp.where(step > 0, total[some, :], 0.0) + term

        @pl.when(step == steps - 1)
        def _():
            out_ref[...] = total[...].astype(BF16)

    block, weight = pl.BlockSpec((tokens, wide), lambda j: (0, j)), pl.BlockSpec((d, wide), lambda j: (0, j))
    like = [jax.ShapeDtypeStruct((tokens, d), BF16)]
    out = pl.BlockSpec((tokens, d), lambda j: (0, 0))
    flops = 4 * tokens * d * ff
    operands, own = [by_gate, by_up, w_gate, w_up], [pltpu.VMEM((tokens, d), F32)]
    return hosting(body, steps, operands, [block, block, weight, weight], like, [out], tasks, identity, flops, 80 * 2**20, own)


def scattered(parts, identity):
    return hosting(None, 6, [], [], [], [], [(parts, (0, 0, 2, 4))], identity, 10**9, 10**8)


def solution(mesh):
    n = mesh.shape["dp"]
    def step(x, dy, *arrays):
        weights, m, v = (arrays[i : i + 3] for i in (0, 3, 6))
        gate, up, down = ([w] for w in weights)
        h0 = x[0]
        a0, gate_w0, up_w0 = gathered(h0, [(gate, (0, 1, 3, 5), 0), (up, (0, 2, 4, 6), 0)], 1)
        tasks = [(down, (0, 6, 16, 20), 0), (gate, (0, 11, 20, 21), 1)]
        gate0, up0, hid0, down_w0, gate_w1 = hidden(a0, gate_w0, up_w0, tasks, 2, 2)
        h1, a1, up_w1 = lowered(hid0, down_w0, h0, [(up, (0, 3, 8, 9), 1)], 3)
        gate1, up1, hid1, down_w1 = hidden(a1, gate_w1, up_w1, [(down, (0, 6, 11, 14), 1)], 4)

        by = dy[0]
        down1 = list(by_weight(hid1, by))
        by_gate1, by_up1, *g_down1 = unhidden(by, down_w1, gate1, up1, [(down1, (0, 0, 3, 11))], 5)
        in_gate1 = list(by_weight(a1, by_gate1))
        by_a, *g_gate1 = by_normed(by_gate1, by_up1, gate_w1, up_w1, [(in_gate1, (0, 0, 3, 9))], 6)
        by = by + jax.vjp(normed, h1)[1](by_a)[0]
        in_up1 = list(by_weight(a1, by_up1))
        by_gate0, by_up0, *g_up1 = unhidden(by, down_w0, gate0, up0, [(in_up1, (0, 0, 3, 11))], 7)
        down0 = list(by_weight(hid0, by))
        *in_gate0, g_down0, s_down0 = by_weight(a0, by_gate0, [(down0, (0, 0, 3, 9))], 8)
        *in_up0, g_gate0, s_gate0 = by_weight(a0, by_up0, [(in_gate0, (0, 0, 3, 9))], 9)
        g_up0 = scattered(in_up0, 10)

        both = [[(g_gate0, s_gate0), g_gate1], [g_up0, g_up1], [(g_down0, s_down0), g_down1]]
        pairs = [[one[0] for one in pair] for pair in both]
        total = jnp.sum(everywhere(n, sum(one[1] for pair in both for one in pair)))
        count = n * sum(w.size for w in weights)
        factor = jnp.minimum(1.0, 0.5 * lax.rsqrt(total / count + 1e-30))
        new = []
        for w, mm, vv, pair in zip(weights, m, v, pairs, strict=True):
            g = jnp.stack(pair).astype(F32) * factor
            new.append(adamw(w.astype(F32), mm, vv, g))
        return tuple(one[which] for which in range(3) for one in new)

    states, cut = P(("rep", "dp"), None, None), P(None, "dp", None)
    return jax.shard_map(
        step,
        mesh=mesh,
        in_specs=(states, states) + (cut,) * 9,
        out_specs=(P("rep", "dp", None),) * 9,
        check_vma=False,
    )
```
